32 devices in a mesh: groups: 2 (over x), tensor: 16 (over z, y, core).
Axes of the slice: x: 2, y: 2, z: 4, core: 2. Of those that a mesh axis runs over, the one named last changes fastest.
Arguments:
- tokens: bfloat16 [128, 4096], P(('groups', 'tensor')), parts along dimension 0, may hold values from -6 to 6
- expert_ids: int32 [128, 2], P(('groups', 'tensor')), parts along dimension 0, may hold values from 0 to 7, as said below
- gate_margin: float32 [128], P(('groups', 'tensor')), parts along dimension 0, may hold values from 0 to 2.5
- lengths: int32 [64], P('groups'), parts along dimension 0, may hold values from 1 to 8, 64 in all
- bench_ids: int32 [64], P('groups'), parts along dimension 0, may hold values from 0 to 7
- target: bfloat16 [128, 4096], P(('groups', 'tensor')), parts along dimension 0, may hold values from -3 to 3
- gate_up_weight: bfloat16 [16, 4096, 896], P('tensor'), may hold values from -0.09375 to 0.09375
- down_weight: bfloat16 [16, 448, 4096], P('tensor'), may hold values from -0.1875 to 0.1875
Outputs:
- mixed: bfloat16 [128, 4096], P(('groups', 'tensor')), parts along dimension 0
- load_ratio: float32 [16], P('groups'), parts along dimension 0
- bench_loss: float32 [16], P('groups'), parts along dimension 0
The draws below stay inside these ranges and needn't reach their ends.
There are 2 independent parts, one for each index of `groups`. The reference program is written for one: setup_inputs(seed, part) draws one part's arguments, and reference() takes and returns one part's arrays. A program takes and returns all parts, laid end to end along the dimension named above; an argument that names none is the same for every part. Nothing has to cross between parts.
Inputs may be any that keep to these rules, and one draw needn't show every extreme that they name: `expert_ids`: each row names 2 different experts; every expert is named by some row; among the rows of one index of tensor no expert is named by more than 2 rows, and on the first and the last index of tensor some expert is named by exactly 2 rows. `lengths`: they sum to 64; the longest is exactly 8.
All inputs are finite; a program needn't handle non-finite values.
Results may differ from the reference program's by a relative error of at most 0.008.
Values may be sent and summed in bfloat16 or wider, within the bound.
A program may use at most 64 MiB of HBM per device.

```python
import math
import jax
import jax.numpy as jnp
import numpy as np
from jax import lax

D = 4096
EXPERTS = 8
TOP = 2
HID_DEV = 448
FFN = 896
BLOCKS = 16
TOK_DEV = 4
TOKENS = 64
CAP = 2
SEQS = 32
SEQ_MOST = 8
BENCH = 8
N_TENSOR = 16


def draw_expert_ids(key, part):
    device_count = TOKENS // TOK_DEV
    average = TOK_DEV * TOP // EXPERTS
    span = 2 * (CAP - average) + 1
    device_range = jnp.arange(device_count, dtype=jnp.int32)
    rising = device_range * span // device_count
    order = jax.random.permutation(jax.random.fold_in(key, 11), EXPERTS).astype(jnp.int32)
    first_half = jnp.zeros((EXPERTS,), jnp.int32).at[order[:EXPERTS // 2]].set(1)
    counts = jnp.where(first_half[None, :] > 0, CAP - rising[:, None], 2 * average - CAP + rising[:, None]).astype(jnp.int32)
    ends = jnp.cumsum(counts, axis=1).astype(jnp.int32)
    route_range = jnp.arange(TOK_DEV * TOP, dtype=jnp.int32)
    sorted_ids = jnp.sum((ends[:, None, :] <= route_range[None, :, None]).astype(jnp.int32), axis=2).astype(jnp.int32)
    first_ids = sorted_ids[:, :TOK_DEV]
    second_ids = sorted_ids[:, TOK_DEV:]
    scores = jax.random.randint(jax.random.fold_in(key, 12), (device_count, TOK_DEV), 0, 1 << 20).astype(jnp.int32)
    scores = scores * TOK_DEV + jnp.arange(TOK_DEV, dtype=jnp.int32)[None, :]
    row_order = jnp.argsort(scores, axis=1, stable=True).astype(jnp.int32)
    first_ids = jnp.take_along_axis(first_ids, row_order, axis=1)
    second_ids = jnp.take_along_axis(second_ids, row_order, axis=1)
    flip = jax.random.randint(jax.random.fold_in(key, 13), (device_count, TOK_DEV), 0, 2).astype(jnp.int32)
    lead = jnp.where(flip > 0, second_ids, first_ids)
    follow = jnp.where(flip > 0, first_ids, second_ids)
    return jnp.stack([lead, follow], axis=2).reshape(TOKENS, TOP).astype(jnp.int32)


def plant(array, stream_key, low, top_value):
    spot = [jax.random.randint(jax.random.fold_in(stream_key, axis), (), 0, length) for axis, length in enumerate(array.shape)]
    main_axis = array.shape.index(max(array.shape))
    next_to = spot[:main_axis] + [(spot[main_axis] + 1) % array.shape[main_axis]] + spot[main_axis + 1:]
    return array.at[tuple(spot)].set(low).at[tuple(next_to)].set(top_value)


def levels(key, dims, pieces, low, high):
    gain = 1.0
    for dim, parts in pieces:
        steps = jax.random.uniform(jax.random.fold_in(jax.random.fold_in(key, 6), dim), (parts,), jnp.float32, low / len(pieces), high / len(pieces))
        gain = gain * jnp.repeat(jnp.exp(steps), dims[dim] // parts).reshape((-1,) + (1,) * (len(dims) - 1 - dim))
    return gain


def split_up(amount, total, most, slope):
    portions = [(1 << 20) // math.isqrt(standing ** slope) + 1 for standing in range(2, amount + 1)]
    rest, given = total - most - (amount - 1), [1] * (amount - 1)
    while rest > 0:
        free = [i for i in range(amount - 1) if given[i] < most]
        whole, remaining = sum([portions[i] for i in free]), rest
        for i in free:
            more = min(most - given[i], max(1, remaining * portions[i] // whole), rest)
            given[i] = given[i] + more
            rest = rest - more
    return np.array([most] + given)


def ragged(rng, number_of, total, most, skew):
    if number_of == 2:
        one = jax.random.randint(rng, (), max(1, total - most), min(most, total - 1) + 1)
        return jnp.stack([one, total - one])
    tallies = jnp.asarray(split_up(number_of, total, most, skew), jnp.int32)
    pairs = (number_of - 1) // 2
    donor, receiver = tallies[1:1 + 2 * pairs:2], tallies[2:2 + 2 * pairs:2]
    room = jnp.minimum(donor - 1, most - receiver)
    shifted = jax.random.randint(jax.random.fold_in(rng, 1), (pairs,), 0, 1 << 20) % (room + 1)
    tallies = tallies.at[1:1 + 2 * pairs:2].set(donor - shifted).at[2:2 + 2 * pairs:2].set(receiver + shifted)
    return tallies[jax.random.permutation(jax.random.fold_in(rng, 2), number_of)]


def noise(stream_key, extent, scale, limit, cuts=(), kind=jnp.bfloat16):
    array = jax.random.normal(stream_key, extent, jnp.float32) * scale
    if len(cuts) > 0:
        array = levels(stream_key, extent, cuts, -0.22, 0.18) * array
    return jnp.clip(array, min=-limit, max=limit).astype(kind)


def setup_inputs(seed: int = 0, part: int = 0) -> dict:
    splits = jax.random.split(jax.random.key(seed), 9)
    own_keys = jax.random.split(jax.random.fold_in(splits[8], part), 9)
    return {
        "tokens": noise(own_keys[0], (TOKENS, D), 1.0, 6.0, ((0, 16),)),
        "expert_ids": draw_expert_ids(jax.random.fold_in(jax.random.fold_in(splits[8], part), 71), part),
        "gate_margin": jnp.clip(2.5 * jax.random.uniform(own_keys[2], (TOKENS,), jnp.float32) ** levels(own_keys[2], (TOKENS,), ((0, 16),), -0.2, 0.2), 0.0, 2.5),
        "lengths": ragged(own_keys[3], SEQS, TOKENS, SEQ_MOST, 2).astype(jnp.int32),
        "bench_ids": plant(jax.random.randint(own_keys[4], (SEQS,), 0, BENCH), jax.random.fold_in(own_keys[4], 1), 0, BENCH - 1).astype(jnp.int32),
        "target": noise(own_keys[5], (TOKENS, D), 0.5, 3.0, ((0, 16),)),
        "gate_up_weight": noise(splits[6], (BLOCKS, D, 2 * HID_DEV), D ** -0.5, 0.09375, ((0, 16),)),
        "down_weight": noise(splits[7], (BLOCKS, HID_DEV, D), FFN ** -0.5, 0.1875, ((0, 16),)),
    }


def reference(tokens, expert_ids, gate_margin, lengths, bench_ids, target, gate_up_weight, down_weight):
    token_total = tokens.shape[0]
    model_width = tokens.shape[1]
    group_size = N_TENSOR // EXPERTS
    hidden = down_weight.shape[1]
    slot_limit = N_TENSOR * CAP
    flat_ids = expert_ids.reshape(-1).astype(jnp.int32)
    pair_total = flat_ids.shape[0]

    def one_expert(expert):
        routed = flat_ids == expert
        chosen_pairs = jnp.nonzero(routed, size=slot_limit, fill_value=0)[0].astype(jnp.int32)
        live_slots = (jnp.arange(slot_limit, dtype=jnp.int32) < jnp.sum(routed.astype(jnp.int32))).astype(jnp.float32)
        chosen_rows = tokens[chosen_pairs // TOP]
        start_block = (expert * group_size).astype(jnp.int32)
        gate_blocks = lax.dynamic_slice_in_dim(gate_up_weight, start_block, group_size, 0)
        down_blocks = lax.dynamic_slice_in_dim(down_weight, start_block, group_size, 0)

        def one_block(running, block_weights):
            gate_up_rows = jnp.dot(chosen_rows, block_weights[0], preferred_element_type=jnp.float32)
            activated = (jax.nn.silu(gate_up_rows[:, :hidden]) * gate_up_rows[:, hidden:]).astype(jnp.bfloat16)
            partial_value = jnp.dot(activated, block_weights[1], preferred_element_type=jnp.float32).astype(jnp.bfloat16)
            partial_value = lax.optimization_barrier(partial_value)
            return running + partial_value.astype(jnp.float32), None

        summed, unused = lax.scan(one_block, jnp.zeros((slot_limit, model_width), jnp.float32), (gate_blocks, down_blocks))
        return chosen_pairs, summed * live_slots[:, None]

    pair_index, expert_outs = lax.map(one_expert, jnp.arange(EXPERTS, dtype=jnp.int32))
    per_pair = jnp.zeros((pair_total, model_width), jnp.float32).at[pair_index.reshape(-1)].add(expert_outs.reshape(-1, model_width))
    picked = per_pair.reshape(token_total, TOP, model_width)
    first_weight = jax.nn.sigmoid(gate_margin)[:, None]
    second_weight = jax.nn.sigmoid(-gate_margin)[:, None]
    mixed_exact = first_weight * picked[:, 0] + second_weight * picked[:, 1]
    mixed = mixed_exact.astype(jnp.bfloat16)
    token_loss = jnp.mean(jnp.square(mixed_exact - target.astype(jnp.float32)), axis=1)
    seq_ends = jnp.cumsum(lengths).astype(jnp.int32)
    positions = jnp.arange(token_total, dtype=jnp.int32)
    seq_hot = ((positions[:, None] >= (seq_ends - lengths)[None, :]) & (positions[:, None] < seq_ends[None, :])).astype(jnp.float32)
    bench_hot = (bench_ids[:, None] == jnp.arange(BENCH, dtype=jnp.int32)[None, :]).astype(jnp.float32)
    token_bench = jnp.dot(seq_hot, bench_hot, precision=lax.Precision.HIGHEST)
    bench_loss = jnp.sum(token_loss[:, None] * token_bench, axis=0) / token_total
    counts = jnp.sum((flat_ids[:, None] == jnp.arange(EXPERTS, dtype=jnp.int32)[None, :]).astype(jnp.float32), axis=0)
    load_ratio = counts * (EXPERTS / (TOP * token_total))
    return mixed, load_ratio, bench_loss
```

```python
import functools
import jax
import jax.numpy as jnp
from jax import lax
from jax.experimental import pallas as pl
from jax.experimental.pallas import tpu as pltpu
from jax.sharding import PartitionSpec as P

EXPERTS = 8
TOP = 2
BENCH = 8
F32 = jnp.float32
BF16 = jnp.bfloat16
I32 = jnp.int32


def iota(shape, dim):
    return lax.broadcasted_iota(I32, shape, dim)


def remote(src, dst, send_sem, recv_sem, device):
    return pltpu.make_async_remote_copy(
        src_ref=src,
        dst_ref=dst,
        send_sem=send_sem,
        recv_sem=recv_sem,
        device_id={"tensor": device},
        device_id_type=pl.DeviceIdType.MESH,
    )


def kernel(
    n,
    cap,
    tok_hbm,
    ids_hbm,
    margin_hbm,
    len_hbm,
    bench_hbm,
    target_hbm,
    gu_hbm,
    down_hbm,
    mixed_hbm,
    sums_ref,
    tok,
    ids,
    margin,
    lens,
    bench,
    target,
    gu_w,
    down_w,
    out,
    xbuf,
    psend,
    precv,
    ret,
    rbuf,
    mixed,
    row_send,
    rows_recv,
    in_sem,
    tok_sem,
    w_sem,
    d_sem,
    sem_s,
    sem_r,
    out_sem,
):
    rows, width = tok.shape
    half = width // 2
    hid = down_w.shape[0]
    group = n // EXPERTS
    slots = EXPERTS * cap
    total = n * cap
    me = lax.axis_index("tensor")
    core = lax.rem(me, 2)
    other = 1 - core
    partner = me + 1 - 2 * core
    pair = lax.div(me, 2)
    my_expert = lax.div(me, group)

    tok_cp = pltpu.make_async_copy(tok_hbm, tok, tok_sem.at[0])
    ids_cp = pltpu.make_async_copy(ids_hbm, ids, tok_sem.at[1])
    ids_cp.start()
    tok_cp.start()
    barrier = pltpu.get_barrier_semaphore()

    def greet(i, carry):
        pl.semaphore_signal(
            barrier,
            inc=1,
            device_id={"tensor": lax.rem(me + i, n)},
            device_id_type=pl.DeviceIdType.MESH,
        )
        return carry

    lax.fori_loop(1, n, greet, 0)
    smalls = [
        pltpu.make_async_copy(a, b, in_sem.at[i])
        for i, (a, b) in enumerate(
            ((margin_hbm, margin), (len_hbm, lens), (bench_hbm, bench), (target_hbm, target))
        )
    ]
    for cp in smalls:
        cp.start()
    own_rows = pl.ds(pl.multiple_of(core * half, half), half)
    other_rows = pl.ds(pl.multiple_of(other * half, half), half)
    w_own = pltpu.make_async_copy(gu_hbm.at[0, own_rows], gu_w.at[own_rows], w_sem.at[0])
    w_other = pltpu.make_async_copy(gu_hbm.at[0, other_rows], gu_w.at[other_rows], w_sem.at[1])
    w_down = pltpu.make_async_copy(down_hbm.at[0], down_w, w_sem.at[2])
    w_own.start()
    w_other.start()
    w_down.start()

    ids_cp.wait()
    tok_cp.wait()
    id_rows = ids[...]
    slot_row = iota((slots, 1), 0)
    slot_expert = slot_row // cap
    slot_place = slot_row - slot_expert * cap
    seen = jnp.zeros((slots, 1), I32)
    packed = jnp.zeros((slots, width), F32)
    for t in range(rows):
        hit = (id_rows[t : t + 1, 0:1] == slot_expert) | (id_rows[t : t + 1, 1:2] == slot_expert)
        chosen = jnp.where(hit & (seen == slot_place), 1.0, 0.0).astype(F32)
        packed = packed + chosen * tok[t : t + 1, :].astype(F32)
        seen = seen + jnp.where(hit, 1, 0)
    packed = packed.astype(BF16)
    for e in range(EXPERTS):
        for h in range(2):
            out[h, e] = packed[e * cap : (e + 1) * cap, h * half : (h + 1) * half]
    xbuf[core, me] = out[core, my_expert]

    pl.semaphore_wait(barrier, n - 1)

    def dispatch(i, carry):
        d = lax.rem(me + i, n)
        h = lax.rem(d, 2)
        remote(
            out.at[h, lax.div(d, group)], xbuf.at[h, me], sem_s.at[0], sem_r.at[0], d
        ).start()
        return carry

    lax.fori_loop(1, n, dispatch, 0)

    for cp in smalls:
        cp.wait()
    seqs = lens.shape[1]
    across = iota((seqs, seqs), 1)
    down_axis = iota((seqs, seqs), 0)
    len_row = lens[...]
    len_col = jnp.sum(jnp.where(across == down_axis, len_row, 0).astype(F32), axis=1, keepdims=True)
    ends = jnp.sum(jnp.where(down_axis <= across, len_col, 0.0), axis=0, keepdims=True)
    starts = ends - len_row.astype(F32)
    position = (me * rows + iota((rows, seqs), 0)).astype(F32)
    in_seq = (position >= starts) & (position < ends)
    token_bench = (
        jnp.sum(
            jnp.where(in_seq, bench[...].astype(F32) + 1.0, 0.0), axis=1, keepdims=True
        )
        - 1.0
    )
    lane = iota((rows, 128), 1)
    bench_hot = jnp.where(token_bench == lane.astype(F32), 1.0, 0.0)
    load_hot = jnp.where(
        (id_rows[:, 0:1] + BENCH == lane) | (id_rows[:, 1:2] + BENCH == lane), 1.0, 0.0
    )

    terms = 32
    pairs_rows = total // 2
    col = iota((1, pairs_rows), 1)
    col_expert = (col // cap) // (group // 2)
    col_place = lax.rem(col, cap)
    term_row = iota((terms, pairs_rows), 0)
    weights = jnp.zeros((terms, pairs_rows), F32)
    seen = jnp.zeros((1, pairs_rows), I32)
    for t in range(rows):
        first = id_rows[t : t + 1, 0:1] == col_expert
        second = id_rows[t : t + 1, 1:2] == col_expert
        m = margin[0:1, t : t + 1]
        gate = jnp.where(first, 1.0 / (1.0 + jnp.exp(-m)), 0.0) + jnp.where(
            second, 1.0 / (1.0 + jnp.exp(m)), 0.0
        )
        gate = jnp.where(seen == col_place, gate, 0.0)
        weights = weights + jnp.where(lax.rem(term_row, 8) == t, gate, 0.0)
        seen = seen + jnp.where(first | second, 1, 0)
    high = weights.astype(BF16).astype(F32)
    mid = (weights - high).astype(BF16).astype(F32)
    low = weights - high - mid
    weights = jnp.where(
        term_row < 8,
        high,
        jnp.where(term_row < 16, mid, jnp.where(term_row < 24, low, 0.0)),
    ).astype(BF16)

    remote(xbuf.at[core, pl.ds(0, n - 1)], xbuf.at[core, pl.ds(0, n - 1)], sem_s.at[0], sem_r.at[0], partner).wait_recv()
    forward = remote(xbuf.at[core], xbuf.at[core], sem_s.at[1], sem_r.at[1], partner)
    forward.start()
    w_own.wait()
    x = jnp.concatenate([xbuf[core, i] for i in range(n)], axis=0)
    both = jnp.dot(x, gu_w[own_rows, :], preferred_element_type=F32)
    w_other.wait()
    forward.wait_recv()
    x = jnp.concatenate([xbuf[other, i] for i in range(n)], axis=0)
    both = both + jnp.dot(x, gu_w[other_rows, :], preferred_element_type=F32)
    v = both[:, :hid]
    act = (v / (1.0 + jnp.exp(-v)) * both[:, hid:]).astype(BF16)
    w_down.wait()

    pieces = psend.shape[0]
    piece = half // pieces
    swaps = []
    for j in range(pieces):
        columns = pl.ds(pl.multiple_of(other * half + j * piece, piece), piece)
        psend[j] = jnp.dot(act, down_w[:, columns], preferred_element_type=F32).astype(BF16)
        swap = remote(psend.at[j], precv.at[j], d_sem.at[0, j], d_sem.at[1, j], partner)
        swap.start()
        swaps.append(swap)
    for j in range(pieces):
        columns = pl.ds(pl.multiple_of(core * half + j * piece, piece), piece)
        mine = jnp.dot(act, down_w[:, columns], preferred_element_type=F32)
        swaps[j].wait_recv()
        summed = (mine + precv[j].astype(F32)).astype(BF16)
        for i in range(n):
            ret[i, :, j * piece : (j + 1) * piece] = summed[i * cap : (i + 1) * cap, :]

    def give_back(i, carry):
        d = lax.rem(me + i, n)
        remote(ret.at[d], rbuf.at[core, pair], sem_s.at[2], sem_r.at[2], d).start()
        return carry

    lax.fori_loop(1, n, give_back, 0)
    rbuf[core, pair] = ret[me]
    stand_in = xbuf.at[0, pl.ds(0, n - 1)]
    remote(stand_in, stand_in, sem_s.at[2], sem_r.at[2], partner).wait_recv()

    loss = jnp.zeros((rows, 1), F32)
    for h in range(2):
        got = jnp.concatenate([rbuf[h, i] for i in range(n // 2)], axis=0)
        parts = jnp.dot(weights, got, preferred_element_type=F32)
        exact = (parts[0:8] + parts[8:16] + parts[16:24])[:rows]
        span = slice(h * half, (h + 1) * half)
        mixed[:, span] = exact.astype(BF16)
        gap = exact - target[:, span].astype(F32)
        loss = loss + jnp.sum(gap * gap, axis=1, keepdims=True)
    loss = loss * (1.0 / width)
    mine = jnp.sum(bench_hot * loss + load_hot, axis=0, keepdims=True)
    row_send[0] = mine
    rows_recv[me] = mine

    def share(i, carry):
        remote(
            row_send.at[0], rows_recv.at[me], sem_s.at[3], sem_r.at[3], lax.rem(me + i, n)
        ).start()
        return carry

    lax.fori_loop(1, n, share, 0)
    mixed_cp = pltpu.make_async_copy(mixed, mixed_hbm, out_sem)
    mixed_cp.start()
    remote(stand_in, stand_in, sem_s.at[0], sem_r.at[0], partner).wait_send()
    forward.wait_send()
    for swap in swaps:
        swap.wait_send()
    remote(stand_in, stand_in, sem_s.at[2], sem_r.at[2], partner).wait_send()
    all_rows = rows_recv.at[pl.ds(0, n - 1)]
    shared = remote(all_rows, all_rows, sem_s.at[3], sem_r.at[3], partner)
    shared.wait_recv()
    everyone = jnp.sum(rows_recv[...], axis=0)
    token_total = rows * n
    lane = iota((1, 128), 1)
    sums_ref[...] = everyone * jnp.where(
        lane < BENCH, 1.0 / token_total, EXPERTS / (TOP * token_total)
    )
    shared.wait_send()
    mixed_cp.wait()


def on_device(
    tokens, expert_ids, gate_margin, lengths, bench_ids, target, gate_up_weight, down_weight
):
    n = lax.axis_size("tensor")
    rows, width = tokens.shape
    cap = rows * TOP // EXPERTS + 1
    half = width // 2
    hid = down_weight.shape[1]
    pieces = 2
    seqs = lengths.shape[0]
    hbm = pl.BlockSpec(memory_space=pl.ANY)
    mixed, sums = pl.pallas_call(
        functools.partial(kernel, n, cap),
        out_shape=(
            jax.ShapeDtypeStruct((rows, width), BF16),
            jax.ShapeDtypeStruct((1, 128), F32),
        ),
        in_specs=[hbm] * 8,
        out_specs=(hbm, pl.BlockSpec(memory_space=pltpu.VMEM)),
        scratch_shapes=[
            pltpu.VMEM((rows, width), BF16),
            pltpu.VMEM((rows, TOP), I32),
            pltpu.VMEM((1, rows), F32),
            pltpu.VMEM((1, seqs), I32),
            pltpu.VMEM((1, seqs), I32),
            pltpu.VMEM((rows, width), BF16),
            pltpu.VMEM((width, 2 * hid), BF16),
            pltpu.VMEM((hid, width), BF16),
            pltpu.VMEM((2, EXPERTS, cap, half), BF16),
            pltpu.VMEM((2, n, cap, half), BF16),
            pltpu.VMEM((pieces, n * cap, half // pieces), BF16),
            pltpu.VMEM((pieces, n * cap, half // pieces), BF16),
            pltpu.VMEM((n, cap, half), BF16),
            pltpu.VMEM((2, n // 2, cap, half), BF16),
            pltpu.VMEM((rows, width), BF16),
            pltpu.VMEM((1, 1, 128), F32),
            pltpu.VMEM((n, 1, 128), F32),
            pltpu.SemaphoreType.DMA((4,)),
            pltpu.SemaphoreType.DMA((2,)),
            pltpu.SemaphoreType.DMA((3,)),
            pltpu.SemaphoreType.DMA((2, pieces)),
            pltpu.SemaphoreType.DMA((4,)),
            pltpu.SemaphoreType.DMA((4,)),
            pltpu.SemaphoreType.DMA,
        ],
        compiler_params=pltpu.CompilerParams(
            collective_id=0, has_side_effects=True, vmem_limit_bytes=60 * 1024 * 1024
        ),
    )(
        tokens,
        expert_ids,
        gate_margin.reshape(1, rows),
        lengths.reshape(1, seqs),
        bench_ids.reshape(1, seqs),
        target,
        gate_up_weight,
        down_weight,
    )
    return mixed, sums[0, BENCH : BENCH + EXPERTS], sums[0, :BENCH]


def solution(mesh):
    placed = (
        P(("groups", "tensor"), None),
        P(("groups", "tensor"), None),
        P(("groups", "tensor")),
        P("groups"),
        P("groups"),
        P(("groups", "tensor"), None),
        P("tensor", None, None),
        P("tensor", None, None),
    )
    return jax.shard_map(
        on_device,
        mesh=mesh,
        in_specs=placed,
        out_specs=(P(("groups", "tensor"), None), P("groups"), P("groups")),
        check_vma=False,
    )
```

```python
import functools
import jax
import jax.numpy as jnp
from jax import lax
from jax.experimental import pallas as pl
from jax.experimental.pallas import tpu as pltpu
from jax.sharding import PartitionSpec as P

EXPERTS = 8
TOP = 2
BENCH = 8
F32 = jnp.float32
BF16 = jnp.bfloat16
I32 = jnp.int32


def iota(shape, dim):
    return lax.broadcasted_iota(I32, shape, dim)


def remote(src, dst, send_sem, recv_sem, device):
    return pltpu.make_async_remote_copy(
        src_ref=src,
        dst_ref=dst,
        send_sem=send_sem,
        recv_sem=recv_sem,
        device_id={"tensor": device},
        device_id_type=pl.DeviceIdType.MESH,
    )


def kernel(
    n,
    cap,
    tok_hbm,
    ids_hbm,
    margin_hbm,
    len_hbm,
    bench_hbm,
    target_hbm,
    gu_hbm,
    down_hbm,
    mixed_hbm,
    sums_ref,
    tok,
    ids,
    margin,
    lens,
    bench,
    target,
    gu_w,
    down_w,
    out,
    xbuf,
    psend,
    precv,
    ret,
    rbuf,
    mixed,
    row_send,
    rows_recv,
    in_sem,
    tok_sem,
    w_sem,
    d_sem,
    sem_s,
    sem_r,
    out_sem,
):
    rows, width = tok.shape
    half = width // 2
    hid = down_w.shape[0]
    group = n // EXPERTS
    slots = EXPERTS * cap
    total = n * cap
    me = lax.axis_index("tensor")
    core = lax.rem(me, 2)
    other = 1 - core
    partner = me + 1 - 2 * core
    pair = lax.div(me, 2)
    my_expert = lax.div(me, group)

    flips = [
        (1 - 2 * lax.rem(lax.div(me, 1 << b), 2)) * (1 << b) for b in range((n - 1).bit_length())
    ]
    peers = []
    for i in range(n - 1, 0, -1):
        d = me
        for b, flip in enumerate(flips):
            if (i >> b) & 1:
                d = d + flip
        peers.append(d)

    tok_cp = pltpu.make_async_copy(tok_hbm, tok, tok_sem.at[0])
    ids_cp = pltpu.make_async_copy(ids_hbm, ids, tok_sem.at[1])
    ids_cp.start()
    tok_cp.start()
    barrier = pltpu.get_barrier_semaphore()

    for d in peers:
        pl.semaphore_signal(
            barrier, inc=1, device_id={"tensor": d}, device_id_type=pl.DeviceIdType.MESH
        )
    smalls = [
        pltpu.make_async_copy(a, b, in_sem.at[i])
        for i, (a, b) in enumerate(
            ((margin_hbm, margin), (len_hbm, lens), (bench_hbm, bench), (target_hbm, target))
        )
    ]
    for cp in smalls:
        cp.start()
    own_rows = pl.ds(pl.multiple_of(core * half, half), half)
    other_rows = pl.ds(pl.multiple_of(other * half, half), half)
    w_own = pltpu.make_async_copy(gu_hbm.at[0, own_rows], gu_w.at[own_rows], w_sem.at[0])
    w_other = pltpu.make_async_copy(gu_hbm.at[0, other_rows], gu_w.at[other_rows], w_sem.at[1])
    w_down = pltpu.make_async_copy(down_hbm.at[0], down_w, w_sem.at[2])
    w_own.start()
    w_other.start()
    w_down.start()

    ids_cp.wait()
    tok_cp.wait()
    id_rows = ids[...]
    slot_row = iota((slots, 1), 0)
    slot_expert = slot_row // cap
    slot_place = slot_row - slot_expert * cap
    seen = jnp.zeros((slots, 1), I32)
    packed = jnp.zeros((slots, width), F32)
    for t in range(rows):
        hit = (id_rows[0:1, t : t + 1] == slot_expert) | (id_rows[1:2, t : t + 1] == slot_expert)
        chosen = jnp.where(hit & (seen == slot_place), 1.0, 0.0).astype(F32)
        packed = packed + chosen * tok[t : t + 1, :].astype(F32)
        seen = seen + jnp.where(hit, 1, 0)
    packed = packed.astype(BF16)
    for e in range(EXPERTS):
        for h in range(2):
            out[h, e] = packed[e * cap : (e + 1) * cap, h * half : (h + 1) * half]
    xbuf[core, me] = out[core, my_expert]

    pl.semaphore_wait(barrier, n - 1)

    for d in peers:
        h = lax.rem(d, 2)
        remote(
            out.at[h, lax.div(d, group)], xbuf.at[h, me], sem_s.at[0], sem_r.at[0], d
        ).start()

    for cp in smalls:
        cp.wait()
    seqs = lens.shape[1]
    across = iota((seqs, seqs), 1)
    down_axis = iota((seqs, seqs), 0)
    len_row = lens[...]
    len_col = jnp.sum(jnp.where(across == down_axis, len_row, 0).astype(F32), axis=1, keepdims=True)
    ends = jnp.sum(jnp.where(down_axis <= across, len_col, 0.0), axis=0, keepdims=True)
    starts = ends - len_row.astype(F32)
    position = (me * rows + iota((rows, seqs), 0)).astype(F32)
    in_seq = (position >= starts) & (position < ends)
    token_bench = (
        jnp.sum(
            jnp.where(in_seq, bench[...].astype(F32) + 1.0, 0.0), axis=1, keepdims=True
        )
        - 1.0
    )
    lane = iota((rows, 128), 1)
    bench_hot = jnp.where(token_bench == lane.astype(F32), 1.0, 0.0)
    load_hot = jnp.zeros((1, 128), F32)
    for t in range(rows):
        for k in range(TOP):
            load_hot = load_hot + jnp.where(id_rows[k : k + 1, t : t + 1] + BENCH == lane[0:1], 1.0, 0.0)

    terms = 32
    pairs_rows = total // 2
    col = iota((1, pairs_rows), 1)
    col_expert = (col // cap) // (group // 2)
    col_place = lax.rem(col, cap)
    term_row = iota((terms, pairs_rows), 0)
    weights = jnp.zeros((terms, pairs_rows), F32)
    seen = jnp.zeros((1, pairs_rows), I32)
    for t in range(rows):
        first = id_rows[0:1, t : t + 1] == col_expert
        second = id_rows[1:2, t : t + 1] == col_expert
        m = margin[0:1, t : t + 1]
        gate = jnp.where(first, 1.0 / (1.0 + jnp.exp(-m)), 0.0) + jnp.where(
            second, 1.0 / (1.0 + jnp.exp(m)), 0.0
        )
        gate = jnp.where(seen == col_place, gate, 0.0)
        weights = weights + jnp.where(lax.rem(term_row, 8) == t, gate, 0.0)
        seen = seen + jnp.where(first | second, 1, 0)
    high = weights.astype(BF16).astype(F32)
    mid = (weights - high).astype(BF16).astype(F32)
    low = weights - high - mid
    weights = jnp.where(
        term_row < 8,
        high,
        jnp.where(term_row < 16, mid, jnp.where(term_row < 24, low, 0.0)),
    ).astype(BF16)

    remote(xbuf.at[core, pl.ds(0, n - 1)], xbuf.at[core, pl.ds(0, n - 1)], sem_s.at[0], sem_r.at[0], partner).wait_recv()
    forward = remote(xbuf.at[core], xbuf.at[core], sem_s.at[1], sem_r.at[1], partner)
    forward.start()
    w_own.wait()
    x = jnp.concatenate([xbuf[core, i] for i in range(n)], axis=0)
    both = jnp.dot(x, gu_w[own_rows, :], preferred_element_type=F32)
    w_other.wait()
    forward.wait_recv()
    x = jnp.concatenate([xbuf[other, i] for i in range(n)], axis=0)
    both = both + jnp.dot(x, gu_w[other_rows, :], preferred_element_type=F32)
    v = both[:, :hid]
    act = (v / (1.0 + jnp.exp(-v)) * both[:, hid:]).astype(BF16)
    w_down.wait()

    pieces = psend.shape[0]
    piece = half // pieces
    swaps = []
    for j in range(pieces):
        columns = pl.ds(pl.multiple_of(other * half + j * piece, piece), piece)
        psend[j] = jnp.dot(act, down_w[:, columns], preferred_element_type=F32).astype(BF16)
        swap = remote(psend.at[j], precv.at[j], d_sem.at[0, j], d_sem.at[1, j], partner)
        swap.start()
        swaps.append(swap)
    for j in range(pieces):
        columns = pl.ds(pl.multiple_of(core * half + j * piece, piece), piece)
        mine = jnp.dot(act, down_w[:, columns], preferred_element_type=F32)
        swaps[j].wait_recv()
        summed = (mine + precv[j].astype(F32)).astype(BF16)
        for i in range(n):
            ret[j, i] = summed[i * cap : (i + 1) * cap, :]
        for d in peers:
            remote(
                ret.at[j, d], rbuf.at[core, j, pair], d_sem.at[2, j], d_sem.at[3, j], d
            ).start()
        rbuf[core, j, pair] = ret[j, me]

    stand_in = xbuf.at[0, pl.ds(0, n - 1)]
    returned = []
    for j in range(pieces):
        sent = ret.at[j, pl.ds(0, n - 1)]
        returned.append(remote(sent, sent, d_sem.at[2, j], d_sem.at[3, j], partner))

    loss = jnp.zeros((rows, 1), F32)
    for j in range(pieces):
        returned[j].wait_recv()
        for h in range(2):
            got = jnp.concatenate([rbuf[h, j, i] for i in range(n // 2)], axis=0)
            parts = jnp.dot(weights, got, preferred_element_type=F32)
            exact = (parts[0:8] + parts[8:16] + parts[16:24])[:rows]
            span = slice(h * half + j * piece, h * half + (j + 1) * piece)
            mixed[:, span] = exact.astype(BF16)
            gap = exact - target[:, span].astype(F32)
            loss = loss + jnp.sum(gap * gap, axis=1, keepdims=True)
    loss = loss * (1.0 / width)
    mine = jnp.sum(bench_hot * loss, axis=0, keepdims=True) + load_hot
    row_send[0] = mine
    rows_recv[me] = mine

    for d in peers:
        remote(row_send.at[0], rows_recv.at[me], sem_s.at[3], sem_r.at[3], d).start()
    mixed_cp = pltpu.make_async_copy(mixed, mixed_hbm, out_sem)
    mixed_cp.start()
    remote(stand_in, stand_in, sem_s.at[0], sem_r.at[0], partner).wait_send()
    forward.wait_send()
    for swap in swaps:
        swap.wait_send()
    for back in returned:
        back.wait_send()
    all_rows = rows_recv.at[pl.ds(0, n - 1)]
    shared = remote(all_rows, all_rows, sem_s.at[3], sem_r.at[3], partner)
    shared.wait_recv()
    everyone = jnp.sum(rows_recv[...], axis=0)
    token_total = rows * n
    lane = iota((1, 128), 1)
    sums_ref[...] = everyone * jnp.where(
        lane < BENCH, 1.0 / token_total, EXPERTS / (TOP * token_total)
    )
    shared.wait_send()
    mixed_cp.wait()


def finish(mixed_in, sums_in, mixed_ref, load_ref, loss_ref):
    mixed_ref[...] = mixed_in[...]
    sums = sums_in[...]
    load_ref[...] = sums[:, BENCH : BENCH + EXPERTS]
    loss_ref[...] = sums[:, :BENCH]


def on_device(
    tokens, expert_ids, gate_margin, lengths, bench_ids, target, gate_up_weight, down_weight
):
    n = lax.axis_size("tensor")
    rows, width = tokens.shape
    cap = rows * TOP // EXPERTS + 1
    half = width // 2
    hid = down_weight.shape[1]
    pieces = 2
    seqs = lengths.shape[0]
    hbm = pl.BlockSpec(memory_space=pl.ANY)
    mixed, sums = pl.pallas_call(
        functools.partial(kernel, n, cap),
        out_shape=(
            jax.ShapeDtypeStruct((rows, width), BF16),
            jax.ShapeDtypeStruct((1, 128), F32),
        ),
        in_specs=[hbm] * 8,
        out_specs=(hbm, pl.BlockSpec(memory_space=pltpu.VMEM)),
        scratch_shapes=[
            pltpu.VMEM((rows, width), BF16),
            pltpu.VMEM((TOP, rows), I32),
            pltpu.VMEM((1, rows), F32),
            pltpu.VMEM((1, seqs), I32),
            pltpu.VMEM((1, seqs), I32),
            pltpu.VMEM((rows, width), BF16),
            pltpu.VMEM((width, 2 * hid), BF16),
            pltpu.VMEM((hid, width), BF16),
            pltpu.VMEM((2, EXPERTS, cap, half), BF16),
            pltpu.VMEM((2, n, cap, half), BF16),
            pltpu.VMEM((pieces, n * cap, half // pieces), BF16),
            pltpu.VMEM((pieces, n * cap, half // pieces), BF16),
            pltpu.VMEM((pieces, n, cap, half // pieces), BF16),
            pltpu.VMEM((2, pieces, n // 2, cap, half // pieces), BF16),
            pltpu.VMEM((rows, width), BF16),
            pltpu.VMEM((1, 1, 128), F32),
            pltpu.VMEM((n, 1, 128), F32),
            pltpu.SemaphoreType.DMA((4,)),
            pltpu.SemaphoreType.DMA((2,)),
            pltpu.SemaphoreType.DMA((3,)),
            pltpu.SemaphoreType.DMA((4, pieces)),
            pltpu.SemaphoreType.DMA((4,)),
            pltpu.SemaphoreType.DMA((4,)),
            pltpu.SemaphoreType.DMA,
        ],
        compiler_params=pltpu.CompilerParams(
            collective_id=0, has_side_effects=True, vmem_limit_bytes=60 * 1024 * 1024
        ),
    )(
        tokens,
        expert_ids.T,
        gate_margin.reshape(1, rows),
        lengths.reshape(1, seqs),
        bench_ids.reshape(1, seqs),
        target,
        gate_up_weight,
        down_weight,
    )
    vmem = pl.BlockSpec(memory_space=pltpu.VMEM)
    mixed, load, bench_loss = pl.pallas_call(
        finish,
        out_shape=(
            jax.ShapeDtypeStruct((rows, width), BF16),
            jax.ShapeDtypeStruct((1, EXPERTS), F32),
            jax.ShapeDtypeStruct((1, BENCH), F32),
        ),
        in_specs=[vmem, vmem],
        out_specs=(vmem, vmem, vmem),
    )(mixed, sums)
    return mixed, load.reshape(EXPERTS), bench_loss.reshape(BENCH)


def solution(mesh):
    placed = (
        P(("groups", "tensor"), None),
        P(("groups", "tensor"), None),
        P(("groups", "tensor")),
        P("groups"),
        P("groups"),
        P(("groups", "tensor"), None),
        P("tensor", None, None),
        P("tensor", None, None),
    )
    return jax.shard_map(
        on_device,
        mesh=mesh,
        in_specs=placed,
        out_specs=(P(("groups", "tensor"), None), P("groups"), P("groups")),
        check_vma=False,
    )
```

```python
import functools
import jax
import jax.numpy as jnp
from jax import lax
from jax.experimental import pallas as pl
from jax.experimental.pallas import tpu as pltpu
from jax.sharding import PartitionSpec as P

EXPERTS = 8
TOP = 2
BENCH = 8
F32 = jnp.float32
BF16 = jnp.bfloat16
I32 = jnp.int32


def iota(shape, dim):
    return lax.broadcasted_iota(I32, shape, dim)


def remote(src, dst, send_sem, recv_sem, device):
    return pltpu.make_async_remote_copy(
        src_ref=src,
        dst_ref=dst,
        send_sem=send_sem,
        recv_sem=recv_sem,
        device_id={"tensor": device},
        device_id_type=pl.DeviceIdType.MESH,
    )


def kernel(
    n,
    cap,
    tok_hbm,
    ids_hbm,
    margin_hbm,
    len_hbm,
    bench_hbm,
    target_hbm,
    gu_hbm,
    down_hbm,
    mixed,
    sums_ref,
    tok,
    ids,
    margin,
    lens,
    bench,
    target,
    gu_w,
    down_w,
    out,
    xbuf,
    down_p,
    act_send,
    act_recv,
    ret,
    rbuf,
    row_send,
    rows_recv,
    in_sem,
    tok_sem,
    w_sem,
    d_sem,
    sem_s,
    sem_r,
):
    rows, width = tok.shape
    half = width // 2
    hid = down_w.shape[0]
    group = n // EXPERTS
    slots = EXPERTS * cap
    total = n * cap
    me = lax.axis_index("tensor")
    core = lax.rem(me, 2)
    other = 1 - core
    partner = me + 1 - 2 * core
    pair = lax.div(me, 2)
    my_expert = lax.div(me, group)

    flips = [
        (1 - 2 * lax.rem(lax.div(me, 1 << b), 2)) * (1 << b) for b in range((n - 1).bit_length())
    ]
    peers = []
    for i in range(n - 1, 0, -1):
        d = me
        for b, flip in enumerate(flips):
            if (i >> b) & 1:
                d = d + flip
        peers.append(d)

    tok_cp = pltpu.make_async_copy(tok_hbm, tok, tok_sem.at[0])
    ids_cp = pltpu.make_async_copy(ids_hbm, ids, tok_sem.at[1])
    ids_cp.start()
    tok_cp.start()
    barrier = pltpu.get_barrier_semaphore()

    for d in peers:
        pl.semaphore_signal(
            barrier, inc=1, device_id={"tensor": d}, device_id_type=pl.DeviceIdType.MESH
        )
    smalls = [
        pltpu.make_async_copy(a, b, in_sem.at[i])
        for i, (a, b) in enumerate(
            ((margin_hbm, margin), (len_hbm, lens), (bench_hbm, bench), (target_hbm, target))
        )
    ]
    for cp in smalls:
        cp.start()
    own_rows = pl.ds(pl.multiple_of(core * half, half), half)
    other_rows = pl.ds(pl.multiple_of(other * half, half), half)
    w_own = pltpu.make_async_copy(gu_hbm.at[0, own_rows], gu_w.at[own_rows], w_sem.at[0])
    w_other = pltpu.make_async_copy(gu_hbm.at[0, other_rows], gu_w.at[other_rows], w_sem.at[1])
    own_cols = pl.ds(pl.multiple_of(core * half, half), half)
    other_cols = pl.ds(pl.multiple_of(other * half, half), half)
    w_down = pltpu.make_async_copy(down_hbm.at[0, :, own_cols], down_w, w_sem.at[2])
    w_own.start()
    w_other.start()
    w_down.start()

    ids_cp.wait()
    tok_cp.wait()
    id_rows = ids[...]
    slot_row = iota((slots, 1), 0)
    slot_expert = slot_row // cap
    slot_place = slot_row - slot_expert * cap
    seen = jnp.zeros((slots, 1), I32)
    packed = jnp.zeros((slots, width), F32)
    for t in range(rows):
        hit = (id_rows[0:1, t : t + 1] == slot_expert) | (id_rows[1:2, t : t + 1] == slot_expert)
        chosen = jnp.where(hit & (seen == slot_place), 1.0, 0.0).astype(F32)
        packed = packed + chosen * tok[t : t + 1, :].astype(F32)
        seen = seen + jnp.where(hit, 1, 0)
    packed = packed.astype(BF16)
    for e in range(EXPERTS):
        for h in range(2):
            out[h, e] = packed[e * cap : (e + 1) * cap, h * half : (h + 1) * half]
    xbuf[core, me] = out[core, my_expert]

    pl.semaphore_wait(barrier, n - 1)

    for d in peers:
        h = lax.rem(d, 2)
        remote(
            out.at[h, lax.div(d, group)], xbuf.at[h, me], sem_s.at[0], sem_r.at[0], d
        ).start()
    lend = remote(down_hbm.at[0, :, other_cols], down_p, sem_s.at[2], sem_r.at[2], partner)
    lend.start()

    for cp in smalls:
        cp.wait()
    seqs = lens.shape[1]
    across = iota((seqs, seqs), 1)
    down_axis = iota((seqs, seqs), 0)
    len_row = lens[...]
    len_col = jnp.sum(jnp.where(across == down_axis, len_row, 0).astype(F32), axis=1, keepdims=True)
    ends = jnp.sum(jnp.where(down_axis <= across, len_col, 0.0), axis=0, keepdims=True)
    starts = ends - len_row.astype(F32)
    position = (me * rows + iota((rows, seqs), 0)).astype(F32)
    in_seq = (position >= starts) & (position < ends)
    token_bench = (
        jnp.sum(
            jnp.where(in_seq, bench[...].astype(F32) + 1.0, 0.0), axis=1, keepdims=True
        )
        - 1.0
    )
    lane = iota((rows, 128), 1)
    bench_hot = jnp.where(token_bench == lane.astype(F32), 1.0, 0.0)
    load_hot = jnp.zeros((1, 128), F32)
    for t in range(rows):
        for k in range(TOP):
            load_hot = load_hot + jnp.where(id_rows[k : k + 1, t : t + 1] + BENCH == lane[0:1], 1.0, 0.0)

    terms = 32
    pairs_rows = total // 2
    col = iota((1, pairs_rows), 1)
    col_expert = (col // cap) // (group // 2)
    col_place = lax.rem(col, cap)
    term_row = iota((terms, pairs_rows), 0)
    weights = jnp.zeros((terms, pairs_rows), F32)
    seen = jnp.zeros((1, pairs_rows), I32)
    for t in range(rows):
        first = id_rows[0:1, t : t + 1] == col_expert
        second = id_rows[1:2, t : t + 1] == col_expert
        m = margin[0:1, t : t + 1]
        gate = jnp.where(first, 1.0 / (1.0 + jnp.exp(-m)), 0.0) + jnp.where(
            second, 1.0 / (1.0 + jnp.exp(m)), 0.0
        )
        gate = jnp.where(seen == col_place, gate, 0.0)
        weights = weights + jnp.where(lax.rem(term_row, 8) == t, gate, 0.0)
        seen = seen + jnp.where(first | second, 1, 0)
    high = weights.astype(BF16).astype(F32)
    mid = (weights - high).astype(BF16).astype(F32)
    low = weights - high - mid
    weights = jnp.where(
        term_row < 8,
        high,
        jnp.where(term_row < 16, mid, jnp.where(term_row < 24, low, 0.0)),
    ).astype(BF16)

    remote(xbuf.at[core, pl.ds(0, n - 1)], xbuf.at[core, pl.ds(0, n - 1)], sem_s.at[0], sem_r.at[0], partner).wait_recv()
    forward = remote(xbuf.at[core], xbuf.at[core], sem_s.at[1], sem_r.at[1], partner)
    forward.start()
    w_own.wait()
    x = jnp.concatenate([xbuf[core, i] for i in range(n)], axis=0)
    both = jnp.dot(x, gu_w[own_rows, :], preferred_element_type=F32)
    w_other.wait()
    forward.wait_recv()
    x = jnp.concatenate([xbuf[other, i] for i in range(n)], axis=0)
    both = both + jnp.dot(x, gu_w[other_rows, :], preferred_element_type=F32)
    v = both[:, :hid]
    act = (v / (1.0 + jnp.exp(-v)) * both[:, hid:]).astype(BF16)
    w_down.wait()

    act_send[...] = act
    swap = remote(act_send, act_recv, sem_s.at[4], sem_r.at[4], partner)
    swap.start()
    pieces = ret.shape[0]
    piece = half // pieces
    mine = [
        jnp.dot(act, down_w[:, j * piece : (j + 1) * piece], preferred_element_type=F32)
        for j in range(pieces)
    ]
    swap.wait_recv()
    lend.wait_recv()
    act = act_recv[...]
    for j in range(pieces):
        theirs = jnp.dot(act, down_p[:, j * piece : (j + 1) * piece], preferred_element_type=F32)
        summed = (mine[j] + theirs).astype(BF16)
        for i in range(n):
            ret[j, i] = summed[i * cap : (i + 1) * cap, :]
        for d in peers:
            remote(
                ret.at[j, d], rbuf.at[core, j, pair], d_sem.at[2, j], d_sem.at[3, j], d
            ).start()
        rbuf[core, j, pair] = ret[j, me]

    stand_in = xbuf.at[0, pl.ds(0, n - 1)]
    returned = []
    for j in range(pieces):
        sent = ret.at[j, pl.ds(0, n - 1)]
        returned.append(remote(sent, sent, d_sem.at[2, j], d_sem.at[3, j], partner))

    loss = jnp.zeros((rows, 1), F32)
    for j in range(pieces):
        returned[j].wait_recv()
        for h in range(2):
            got = jnp.concatenate([rbuf[h, j, i] for i in range(n // 2)], axis=0)
            parts = jnp.dot(weights, got, preferred_element_type=F32)
            exact = (parts[0:8] + parts[8:16] + parts[16:24])[:rows]
            span = slice(h * half + j * piece, h * half + (j + 1) * piece)
            mixed[:, span] = exact.astype(BF16)
            gap = exact - target[:, span].astype(F32)
            loss = loss + jnp.sum(gap * gap, axis=1, keepdims=True)
    loss = loss * (1.0 / width)
    mine = jnp.sum(bench_hot * loss, axis=0, keepdims=True) + load_hot
    row_send[0] = mine
    rows_recv[me] = mine

    for d in peers:
        remote(row_send.at[0], rows_recv.at[me], sem_s.at[3], sem_r.at[3], d).start()
    remote(stand_in, stand_in, sem_s.at[0], sem_r.at[0], partner).wait_send()
    forward.wait_send()
    swap.wait_send()
    lend.wait_send()
    for back in returned:
        back.wait_send()
    all_rows = rows_recv.at[pl.ds(0, n - 1)]
    shared = remote(all_rows, all_rows, sem_s.at[3], sem_r.at[3], partner)
    shared.wait_recv()
    everyone = jnp.sum(rows_recv[...], axis=0)
    token_total = rows * n
    lane = iota((1, 128), 1)
    sums_ref[...] = everyone * jnp.where(
        lane < BENCH, 1.0 / token_total, EXPERTS / (TOP * token_total)
    )
    shared.wait_send()


def finish(mixed_in, sums_in, mixed_ref, load_ref, loss_ref):
    mixed_ref[...] = mixed_in[...]
    sums = sums_in[...]
    load_ref[...] = sums[:, BENCH : BENCH + EXPERTS]
    loss_ref[...] = sums[:, :BENCH]


def on_device(
    tokens, expert_ids, gate_margin, lengths, bench_ids, target, gate_up_weight, down_weight
):
    n = lax.axis_size("tensor")
    rows, width = tokens.shape
    cap = rows * TOP // EXPERTS + 1
    half = width // 2
    hid = down_weight.shape[1]
    pieces = 2
    seqs = lengths.shape[0]
    hbm = pl.BlockSpec(memory_space=pl.ANY)
    mixed, sums = pl.pallas_call(
        functools.partial(kernel, n, cap),
        out_shape=(
            pltpu.VMEM((rows, width), BF16),
            pltpu.VMEM((1, 128), F32),
        ),
        in_specs=[hbm] * 8,
        out_specs=(pl.BlockSpec(memory_space=pltpu.VMEM), pl.BlockSpec(memory_space=pltpu.VMEM)),
        scratch_shapes=[
            pltpu.VMEM((rows, width), BF16),
            pltpu.VMEM((TOP, rows), I32),
            pltpu.VMEM((1, rows), F32),
            pltpu.VMEM((1, seqs), I32),
            pltpu.VMEM((1, seqs), I32),
            pltpu.VMEM((rows, width), BF16),
            pltpu.VMEM((width, 2 * hid), BF16),
            pltpu.VMEM((hid, half), BF16),
            pltpu.VMEM((2, EXPERTS, cap, half), BF16),
            pltpu.VMEM((2, n, cap, half), BF16),
            pltpu.VMEM((hid, half), BF16),
            pltpu.VMEM((n * cap, hid), BF16),
            pltpu.VMEM((n * cap, hid), BF16),
            pltpu.VMEM((pieces, n, cap, half // pieces), BF16),
            pltpu.VMEM((2, pieces, n // 2, cap, half // pieces), BF16),
            pltpu.VMEM((1, 1, 128), F32),
            pltpu.VMEM((n, 1, 128), F32),
            pltpu.SemaphoreType.DMA((4,)),
            pltpu.SemaphoreType.DMA((2,)),
            pltpu.SemaphoreType.DMA((3,)),
            pltpu.SemaphoreType.DMA((4, pieces)),
            pltpu.SemaphoreType.DMA((5,)),
            pltpu.SemaphoreType.DMA((5,)),
        ],
        compiler_params=pltpu.CompilerParams(
            collective_id=0, has_side_effects=True, vmem_limit_bytes=60 * 1024 * 1024
        ),
    )(
        tokens,
        expert_ids.T,
        gate_margin.reshape(1, rows),
        lengths.reshape(1, seqs),
        bench_ids.reshape(1, seqs),
        target,
        gate_up_weight,
        down_weight,
    )
    vmem = pl.BlockSpec(memory_space=pltpu.VMEM)
    mixed, load, bench_loss = pl.pallas_call(
        finish,
        out_shape=(
            jax.ShapeDtypeStruct((rows, width), BF16),
            jax.ShapeDtypeStruct((1, EXPERTS), F32),
            jax.ShapeDtypeStruct((1, BENCH), F32),
        ),
        in_specs=[vmem, vmem],
        out_specs=(vmem, vmem, vmem),
    )(
        pltpu.with_memory_space_constraint(mixed, pltpu.VMEM),
        pltpu.with_memory_space_constraint(sums, pltpu.VMEM),
    )
    return mixed, load.reshape(EXPERTS), bench_loss.reshape(BENCH)


def solution(mesh):
    placed = (
        P(("groups", "tensor"), None),
        P(("groups", "tensor"), None),
        P(("groups", "tensor")),
        P("groups"),
        P("groups"),
        P(("groups", "tensor"), None),
        P("tensor", None, None),
        P("tensor", None, None),
    )
    return jax.shard_map(
        on_device,
        mesh=mesh,
        in_specs=placed,
        out_specs=(P(("groups", "tensor"), None), P("groups"), P("groups")),
        check_vma=False,
    )
```
